32 devices in a mesh: chan: 8 (over z, x), split: 4 (over y, core).
Axes of the slice: x: 2, y: 2, z: 4, core: 2. Of those that a mesh axis runs over, the one named last changes fastest.
Arguments:
- interaction: bfloat16 [16384, 2048], P(('chan', 'split')), may hold values from -6 to 6
- generator: bfloat16 [16384, 2048], P(('chan', 'split')), may hold values from -0.25 to 0.25
- recoupling: bfloat16 [16384, 2048], P(('chan', 'split')), may hold values from -0.125 to 0.125
- send_order: int32 [16384], P(('chan', 'split')), may hold values from 0 to 511, as said below
- receive_order: int32 [16384], P(('chan', 'split')), may hold values from 0 to 511, as said below
- occupation: int32 [2, 16384], P(None, ('chan', 'split')), may hold values from 0 to 1, as said below
- partner: int32 [2048], replicated, may hold values from 0 to 2047, as said below
Outputs:
- flow: bfloat16 [16384, 2048], P(('chan', 'split'))
The draws below stay inside these ranges and needn't reach their ends.
Inputs may be any that keep to these rules, and one draw needn't show every extreme that they name: `send_order`: within each aligned block of 512 entries, a permutation of 0 to 511. `receive_order`: within each aligned block of 512 entries, a permutation of 0 to 511. `occupation`: in each aligned block of 512 columns exactly 256 columns have unequal entries in the two rows. A pairing of the 2048 columns: partner[partner[k]] = k and partner[k] != k.
All inputs are finite; a program needn't handle non-finite values.
Results may differ from the reference program's by a relative error of at most 0.0066.
Values may be sent and summed in bfloat16 or wider, within the bound.
No kernel may reach another device: no remote copies, remote signals or barrier semaphores. Data moves between devices by JAX's collectives and lax.ppermute only.
A program may use at most 128 MiB of HBM per device.

```python
import jax
import jax.numpy as jnp
from jax import lax

Q = 2048
ROWS_DEV = 512
PAIR_ROWS = 16384
PANELS = 32
N_CHAN = 8
N_SPLIT = 4


def block_permutations(key, salt):
    keys = jax.random.split(jax.random.fold_in(key, salt), PANELS)
    return jax.vmap(lambda one_key: jax.random.permutation(one_key, ROWS_DEV))(keys).astype(jnp.int32)


def draw_send_order(key, part):
    return block_permutations(key, 11).reshape(-1)


def draw_receive_order(key, part):
    return block_permutations(key, 23).reshape(-1)


def draw_occupation(key, part):
    ranks = block_permutations(key, 37)
    active = ranks < ROWS_DEV // 2
    first_bits = jax.random.randint(jax.random.fold_in(key, 41), (PANELS, ROWS_DEV), 0, 2)
    second_bits = jax.random.randint(jax.random.fold_in(key, 43), (PANELS, ROWS_DEV), 0, 2)
    upper = jnp.where(active, first_bits, second_bits)
    lower = jnp.where(active, 1 - first_bits, second_bits)
    return jnp.stack([upper.reshape(-1), lower.reshape(-1)]).astype(jnp.int32)


def draw_partner(key, part):
    shuffled = jax.random.permutation(jax.random.fold_in(key, 53), Q).astype(jnp.int32)
    first_half = shuffled[0::2]
    second_half = shuffled[1::2]
    paired = jnp.zeros((Q,), jnp.int32).at[first_half].set(second_half)
    return paired.at[second_half].set(first_half)


def shard_levels(key, dims, shards, low, top_value):
    gain, own = 1.0, jax.random.fold_in(key, 6)
    for dim, blocks in shards:
        steps = jnp.exp(jax.random.uniform(jax.random.fold_in(own, dim), (blocks,), jnp.float32, low / len(shards), top_value / len(shards)))
        gain = gain * jnp.repeat(steps, dims[dim] // blocks).reshape([-1 if axis == dim else 1 for axis in range(len(dims))])
    return gain


def bell_draw(key, shape, spread, most, shards=(), held_as=jnp.bfloat16):
    drawn = spread * jax.random.normal(key, shape, jnp.float32)
    if shards:
        drawn = drawn * shard_levels(key, shape, shards, -0.22, 0.18)
    return jnp.clip(drawn, -most, most).astype(held_as)


def setup_inputs(seed: int = 0) -> dict:
    key_list = jax.random.split(jax.random.key(seed), 8)
    interaction = bell_draw(key_list[0], (PAIR_ROWS, Q), 1.0, 6.0, ((0, 32),))
    generator = bell_draw(key_list[1], (PAIR_ROWS, Q), (32.0 / Q), 0.25, ((0, 32),))
    recoupling = bell_draw(key_list[2], (PAIR_ROWS, Q), Q ** -0.5, 0.125, ((0, 32),))
    send_order = draw_send_order(jax.random.fold_in(key_list[7], 71), 0)
    receive_order = draw_receive_order(jax.random.fold_in(key_list[7], 71), 0)
    occupation = draw_occupation(jax.random.fold_in(key_list[7], 71), 0)
    partner = draw_partner(jax.random.fold_in(key_list[7], 71), 0)
    return dict(interaction=interaction, generator=generator, recoupling=recoupling, send_order=send_order, receive_order=receive_order, occupation=occupation, partner=partner)


def pick_rows(blocks, order):
    return jax.vmap(jax.vmap(lambda block, picks: block[picks]))(blocks, order)


def place_rows(blocks, order):
    return jax.vmap(jax.vmap(lambda block, picks: jnp.zeros_like(block).at[picks].set(block)))(blocks, order)


def swap_owners(blocks, row_count, per_peer):
    moved = blocks.reshape(N_CHAN, N_SPLIT, N_CHAN, per_peer, Q).transpose(2, 1, 0, 3, 4)
    return moved.reshape(N_CHAN, N_SPLIT, row_count, Q)


def reference(interaction, generator, recoupling, send_order, receive_order, occupation, partner):
    row_count = Q // N_SPLIT
    per_peer = row_count // N_CHAN
    send_blocks = send_order.reshape(N_CHAN, N_SPLIT, row_count).astype(jnp.int32)
    receive_blocks = receive_order.reshape(N_CHAN, N_SPLIT, row_count).astype(jnp.int32)

    def forward(matrix):
        blocks = pick_rows(matrix.reshape(N_CHAN, N_SPLIT, row_count, Q), send_blocks)
        blocks = swap_owners(blocks, row_count, per_peer)
        return pick_rows(blocks, receive_blocks).reshape(N_CHAN, Q, Q)

    routed_pair = forward(interaction)
    routed_generator = forward(generator)
    sixj_all = recoupling.reshape(N_CHAN, Q, Q)
    weight_all = (occupation[0] - occupation[1]).astype(jnp.float32).reshape(N_CHAN, Q)

    def channel(operands):
        pair_block, generator_block, sixj_matrix, weight = operands
        cross_pair = jnp.dot(pair_block, sixj_matrix, preferred_element_type=jnp.float32).astype(jnp.bfloat16)
        cross_generator = jnp.dot(generator_block, sixj_matrix, preferred_element_type=jnp.float32).astype(jnp.bfloat16)
        weight_row = weight.astype(jnp.bfloat16)[None, :]
        commutator = jnp.dot(cross_generator * weight_row, cross_pair, preferred_element_type=jnp.float32)
        commutator = commutator - jnp.dot(cross_pair * weight_row, cross_generator, preferred_element_type=jnp.float32)
        commutator = commutator.astype(jnp.bfloat16)
        recoupled = lax.dot_general(commutator, sixj_matrix, (((1,), (1,)), ((), ())), preferred_element_type=jnp.float32)
        return recoupled.astype(jnp.bfloat16)

    recoupled = lax.map(channel, (routed_pair, routed_generator, sixj_all, weight_all))
    blocks = place_rows(recoupled.reshape(N_CHAN, N_SPLIT, row_count, Q), receive_blocks)
    blocks = swap_owners(blocks, row_count, per_peer)
    restored = place_rows(blocks, send_blocks).reshape(N_CHAN * Q, Q)
    flow = restored.astype(jnp.float32) - restored[:, partner].astype(jnp.float32)
    return flow.astype(jnp.bfloat16)
```

```python
import functools

import jax
import jax.numpy as jnp
from jax import lax
from jax.experimental import pallas as pl
from jax.experimental.pallas import tpu as pltpu
from jax.sharding import PartitionSpec as P


BF = jnp.bfloat16
F32 = jnp.float32
VMEM = pl.BlockSpec(memory_space=pltpu.VMEM)
PARAMS = pltpu.CompilerParams(vmem_limit_bytes=58 * 2**20)


def nn(a, b):
    return jnp.dot(a, b, preferred_element_type=F32)


def nt(a, b):
    return lax.dot_general(a, b, (((1,), (1,)), ((), ())), preferred_element_type=F32)


def tn(a, b):
    return lax.dot_general(a, b, (((0,), (0,)), ((), ())), preferred_element_type=F32)


def one_if(cond):
    return jnp.where(cond, 1.0, 0.0).astype(BF)


def iota(shape, dim):
    return lax.broadcasted_iota(jnp.int32, shape, dim)


def swap(x, axis, bit, size):
    return lax.ppermute(x, axis, [(k, k ^ bit) for k in range(size)])


def send_body(n_chan, order_ref, rows_ref, *refs):
    outs, (pick, moved) = refs[:n_chan], refs[n_chan:]
    rows = rows_ref.shape[0]
    per = rows // n_chan
    me = lax.axis_index("chan")

    @pl.when(pl.program_id(0) == 0)
    def _():
        pick[...] = one_if(iota((rows, rows), 0) == order_ref[...])

    moved[...] = tn(pick[...], rows_ref[...]).astype(BF)
    for r in range(n_chan):
        start = pl.multiple_of(lax.bitwise_xor(me, r) * per, per)
        outs[r][...] = moved[pl.ds(start, per), :]


def send_rows(order, matrix, n_chan, tiles=4):
    rows, q = matrix.shape
    per, tile = rows // n_chan, q // tiles
    return pl.pallas_call(
        functools.partial(send_body, n_chan),
        grid=(tiles,),
        in_specs=[
            pl.BlockSpec((1, rows), lambda n: (0, 0)),
            pl.BlockSpec((rows, tile), lambda n: (0, n)),
        ],
        out_specs=[pl.BlockSpec((per, tile), lambda n: (0, n))] * n_chan,
        out_shape=[jax.ShapeDtypeStruct((per, q), BF)] * n_chan,
        scratch_shapes=[pltpu.VMEM((rows, rows), BF), pltpu.VMEM((rows, tile), BF)],
        compiler_params=PARAMS,
        name="send_rows",
    )(order, matrix)


def pair_body(partner_ref, pairs_ref, count):
    q = partner_ref.shape[1]
    half, step = q // 2, 256
    partner = partner_ref[...]
    column = iota((1, q), 1)
    first = one_if(column < partner)
    lead = jnp.minimum(column, partner)
    count[...] = jnp.zeros_like(count)
    for at in range(0, q, step):
        below = one_if(iota((step, q), 0) + at <= lead)
        count[...] += nn(jnp.broadcast_to(first[:, at : at + step], (8, step)), below)
    rank = count[0:1, :].astype(jnp.int32) - 1
    sign = jnp.where(column < partner, 1.0, -1.0)
    for at in range(0, half, step):
        pairs_ref[at : at + step, :] = jnp.where(iota((step, q), 0) + at == rank, sign, 0.0).astype(BF)


def pair_matrix(partner):
    q = partner.shape[1]
    return pl.pallas_call(
        pair_body,
        in_specs=[VMEM],
        out_specs=VMEM,
        out_shape=jax.ShapeDtypeStruct((q // 2, q), BF),
        scratch_shapes=[pltpu.VMEM((8, q), F32)],
        compiler_params=PARAMS,
        name="pair_matrix",
    )(partner)


def piece_rows(piece, rows):
    t, offset = piece
    me = lax.axis_index("split")
    return pl.multiple_of(lax.bitwise_xor(me, t) * rows + offset, 128)


def early_body(pieces, rows, pairs_ref, *refs):
    blocks, out = refs[:-1], refs[-1]
    half, q = out.shape
    tile = 512

    def step(n, _):
        at = pl.ds(pl.multiple_of(n * tile, tile), tile)
        total = jnp.zeros((half, tile), F32)
        for piece, block in zip(pieces, blocks):
            here = pl.ds(piece_rows(piece, rows), block.shape[0])
            total += nn(pairs_ref[:, here], block[:, at])
        out[:, at] = total.astype(BF)
        return 0

    lax.fori_loop(0, q // tile, step, 0)


def early_pairs(pieces, rows, pairs, blocks):
    half, q = pairs.shape
    return pl.pallas_call(
        functools.partial(early_body, pieces, rows),
        in_specs=[VMEM] * (1 + len(blocks)),
        out_specs=VMEM,
        out_shape=jax.ShapeDtypeStruct((half, q), BF),
        compiler_params=PARAMS,
        name="early_pairs",
    )(pairs, *blocks)


def mix_body(early, late, rows, n_split, pairs_ref, part_ref, weight_ref, *refs):
    blocks = refs[: len(early) + len(late)]
    active_ref, mixed_ref, diff, choose = refs[len(early) + len(late) :]
    half, q = part_ref.shape
    tile = 512
    keep = rows // 2
    me = lax.axis_index("split")

    weight = weight_ref[...]
    mask = jnp.where(weight == 0, 0.0, 1.0)
    upto = one_if(iota((rows, rows), 0) <= iota((rows, rows), 1))
    rank = nn(mask.astype(BF), upto).astype(jnp.int32) - 1
    for t in range(n_split):
        hit = jnp.logical_and(iota((keep, rows), 0) == rank[t : t + 1, :], mask[t : t + 1, :] > 0)
        choose[t] = jnp.where(hit, weight[t : t + 1, :].astype(F32), 0.0).astype(BF)

    def step(n, _):
        at = pl.ds(pl.multiple_of(n * tile, tile), tile)
        total = part_ref[:, at].astype(F32)
        for piece, block in zip(late, blocks[len(early) :]):
            here = pl.ds(piece_rows(piece, rows), block.shape[0])
            total += nn(pairs_ref[:, here], block[:, at])
        diff[:, at] = total.astype(BF)
        return 0

    lax.fori_loop(0, q // tile, step, 0)
    for piece, block in zip(early + late, blocks):
        here = pl.ds(piece_rows(piece, rows), block.shape[0])
        for t in range(n_split):
            column = pl.ds(pl.multiple_of(lax.bitwise_xor(me, t) * rows, rows), rows)
            active_ref[here, t * keep : (t + 1) * keep] = nt(block[:, column], choose[t]).astype(BF)

        def mix(n, _, here=here, block=block):
            at = pl.ds(pl.multiple_of(n * tile, tile), tile)
            mixed_ref[here, at] = nt(block[...], diff[at, :]).astype(BF)
            return 0

        lax.fori_loop(0, half // tile, mix, 0)


def mix_matrices(early, late, rows, n_split, pairs, part, weights, blocks):
    half, q = pairs.shape
    return pl.pallas_call(
        functools.partial(mix_body, early, late, rows, n_split),
        in_specs=[VMEM] * (3 + len(blocks)),
        out_specs=[VMEM, VMEM],
        out_shape=[jax.ShapeDtypeStruct((q, half), BF)] * 2,
        scratch_shapes=[pltpu.VMEM((half, q), BF), pltpu.VMEM((n_split, rows // 2, rows), BF)],
        compiler_params=PARAMS,
        name="mix_matrices",
    )(pairs, part, weights, *blocks)


def cross_body(n_chan, order_ref, weight_ref, active_ref, mixed_ref, *refs):
    blocks = refs[:n_chan]
    cross_ref, rows_ref, arrived, pick = refs[n_chan:]
    rows = arrived.shape[0]
    per, keep = rows // n_chan, rows // 2

    @pl.when(pl.program_id(0) == 0)
    def _():
        for r in range(n_chan):
            arrived[r * per : (r + 1) * per, :] = blocks[r][...]
        me = lax.axis_index("chan")
        slot = order_ref[...]
        relative = lax.bitwise_xor(slot // per, me) * per + slot % per
        place = one_if(iota((rows, rows), 0) == relative)
        mask = jnp.where(weight_ref[...] == 0, 0.0, 1.0)
        upto = one_if(iota((rows, rows), 0) <= iota((rows, rows), 1))
        rank = nn(jnp.broadcast_to(mask, (8, rows)).astype(BF), upto).astype(jnp.int32)[0:1, :] - 1
        hit = jnp.logical_and(iota((keep, rows), 0) == rank, mask > 0)
        pick[...] = nt(one_if(hit), place).astype(BF)

    cross_ref[...] = nn(arrived[...], active_ref[...]).astype(BF)
    rows_ref[...] = nn(pick[...], nn(arrived[...], mixed_ref[...]).astype(BF)).astype(BF)


def cross_rows(order, weight, active, mixed, blocks, tiles=2):
    n_chan = len(blocks)
    q, half = active.shape
    rows = order.shape[1]
    tile = half // tiles
    fixed = lambda n: (0, 0)
    return pl.pallas_call(
        functools.partial(cross_body, n_chan),
        grid=(tiles,),
        in_specs=[pl.BlockSpec((1, rows), fixed)] * 2
        + [pl.BlockSpec((q, tile), lambda n: (0, n))] * 2
        + [pl.BlockSpec((rows // n_chan, q), fixed)] * n_chan,
        out_specs=[
            pl.BlockSpec((rows, tile), lambda n: (0, n)),
            pl.BlockSpec((rows // 2, tile), lambda n: (0, n)),
        ],
        out_shape=[jax.ShapeDtypeStruct((rows, half), BF), jax.ShapeDtypeStruct((rows // 2, half), BF)],
        scratch_shapes=[pltpu.VMEM((rows, q), BF), pltpu.VMEM((rows // 2, rows), BF)],
        compiler_params=PARAMS,
        name="cross_rows",
    )(order, weight, active, mixed, *blocks)


def commute_body(n_chan, n_split, generator_ref, pair_ref, *refs):
    generator_rows, pair_rows = refs[:n_split], refs[n_split : 2 * n_split]
    outs = refs[2 * n_split :]
    rows = generator_ref.shape[0]
    per, keep = rows // n_chan, rows // 2
    total = jnp.zeros((rows, outs[0].shape[1]), F32)
    for t in range(n_split):
        at = slice(t * keep, (t + 1) * keep)
        total += nn(generator_ref[:, at], pair_rows[t][...]) - nn(pair_ref[:, at], generator_rows[t][...])
    total = total.astype(BF)
    for r in range(n_chan):
        outs[r][...] = total[r * per : (r + 1) * per, :]


def commute(generator, pair, generator_rows, pair_rows, n_chan, tiles=2):
    rows, half = generator.shape
    n_split = len(pair_rows)
    width = pair_rows[0].shape[1]
    tile = width // tiles
    return pl.pallas_call(
        functools.partial(commute_body, n_chan, n_split),
        grid=(tiles,),
        in_specs=[pl.BlockSpec((rows, half), lambda n: (0, 0))] * 2
        + [pl.BlockSpec((rows // 2, tile), lambda n: (0, n))] * (2 * n_split),
        out_specs=[pl.BlockSpec((rows // n_chan, tile), lambda n: (0, n))] * n_chan,
        out_shape=[jax.ShapeDtypeStruct((rows // n_chan, width), BF)] * n_chan,
        compiler_params=PARAMS,
        name="commute",
    )(generator, pair, *generator_rows, *pair_rows)


def restore_body(n_chan, order_ref, pairs_ref, *refs):
    blocks, out, restored = refs[:n_chan], refs[n_chan], refs[n_chan + 1]
    rows = out.shape[0]
    per = rows // n_chan

    @pl.when(pl.program_id(0) == 0)
    def _():
        me = lax.axis_index("chan")
        place = one_if(iota((rows, rows), 0) == order_ref[...])
        for r in range(n_chan):
            start = pl.multiple_of(lax.bitwise_xor(me, r) * per, per)
            restored[pl.ds(start, per), :] = blocks[r][...]
        restored[...] = nn(place, restored[...]).astype(BF)

    out[...] = nn(restored[...], pairs_ref[...]).astype(BF)


def restore(order, pairs, blocks, tiles=4):
    n_chan = len(blocks)
    per, half = blocks[0].shape
    q = pairs.shape[1]
    rows = per * n_chan
    tile = q // tiles
    fixed = lambda n: (0, 0)
    return pl.pallas_call(
        functools.partial(restore_body, n_chan),
        grid=(tiles,),
        in_specs=[pl.BlockSpec((1, rows), fixed), pl.BlockSpec((half, tile), lambda n: (0, n))]
        + [pl.BlockSpec((per, half), fixed)] * n_chan,
        out_specs=pl.BlockSpec((rows, tile), lambda n: (0, n)),
        out_shape=jax.ShapeDtypeStruct((rows, q), BF),
        scratch_shapes=[pltpu.VMEM((rows, half), BF)],
        compiler_params=PARAMS,
        name="restore",
    )(order, pairs, *blocks)


def local(n_chan, n_split, interaction, generator, recoupling, send_order, receive_order, occupation, partner):
    rows, q = interaction.shape
    order_out, order_in = send_order[None, :], receive_order[None, :]
    partner = partner[None, :]
    weight = occupation[0:1] - occupation[1:2]
    far = sorted(range(1, n_chan), reverse=True)

    cut = rows // 2
    early = ((0, 0), (1, 0))
    late = tuple((t, at) for at in range(0, rows, cut) for t in range(2, n_split))
    held = {(0, 0): recoupling, (1, 0): swap(recoupling, "split", 1, n_split)}
    for at in range(0, rows, cut):
        for t in range(2, n_split, 2):
            held[(t, at)] = swap(recoupling[at : at + cut], "split", t, n_split)
            held[(t + 1, at)] = swap(held[(t, at)], "split", 1, n_split)
    weights = {0: weight}
    for t in range(1, n_split):
        weights[t] = swap(weight, "split", t, n_split)
    weights = jnp.concatenate([weights[t] for t in range(n_split)] + [jnp.zeros((8 - n_split, rows), jnp.int32)])

    def exchange(blocks):
        arrived = {0: blocks[0]}
        for r in far:
            arrived[r] = swap(blocks[r], "chan", r, n_chan)
        return [arrived[r] for r in range(n_chan)]

    def gather_rows(block):
        held = {0: block}
        for t in range(2, n_split, 2):
            held[t] = swap(block, "split", t, n_split)
        for t in range(0, n_split, 2):
            held[t + 1] = swap(held[t], "split", 1, n_split)
        return [held[t] for t in range(n_split)]

    generator_blocks = exchange(send_rows(order_out, generator, n_chan))
    pair_blocks = exchange(send_rows(order_out, interaction, n_chan))
    pairs = pair_matrix(partner)
    part = early_pairs(early, rows, pairs, [held[p] for p in early])
    active, mixed = mix_matrices(early, late, rows, n_split, pairs, part, weights, [held[p] for p in early + late])
    cross_generator, generator_mine = cross_rows(order_in, weight, active, mixed, generator_blocks)
    generator_rows = gather_rows(generator_mine)
    cross_pair, pair_mine = cross_rows(order_in, weight, active, mixed, pair_blocks)
    pair_rows = gather_rows(pair_mine)
    outgoing = commute(cross_generator, cross_pair, generator_rows, pair_rows, n_chan)
    return restore(order_out, pairs, exchange(outgoing))


def solution(mesh):
    placed = (
        P(("chan", "split"), None),
        P(("chan", "split"), None),
        P(("chan", "split"), None),
        P(("chan", "split")),
        P(("chan", "split")),
        P(None, ("chan", "split")),
        P(),
    )
    return jax.shard_map(
        functools.partial(local, mesh.shape["chan"], mesh.shape["split"]),
        mesh=mesh,
        in_specs=placed,
        out_specs=P(("chan", "split"), None),
        check_vma=False,
    )
```
